8 devices in a mesh: dp: 2 (over z, y), sp: 4 (over x, core).
Axes of the slice: x: 2, y: 2, z: 1, core: 2. Of those that a mesh axis runs over, the one named last changes fastest.
Arguments:
- x_in: bfloat16 [16, 4096, 1152], P('dp', 'sp'), parts along dimension 0
- dy_in: bfloat16 [16, 4096, 1152], P('dp', 'sp'), parts along dimension 0
- positions: int32 [8192], P(('dp', 'sp')), parts along dimension 0
- w_q: bfloat16 [1152, 1024], replicated
- w_k: bfloat16 [1152, 256], replicated
- w_v: bfloat16 [1152, 256], replicated
- w_o: bfloat16 [1024, 1152], replicated
- w_pre: float32 [1152], replicated
- w_post: float32 [1152], replicated
- q_norm: float32 [256], replicated
- k_norm: float32 [256], replicated
Outputs:
- output 1: bfloat16 [16, 4096, 1152], P('dp', 'sp'), parts along dimension 0
- output 2: bfloat16 [16, 4096, 1152], P('dp', 'sp'), parts along dimension 0
- output 3: bfloat16 [2304, 1024], P('dp'), parts along dimension 0
- output 4: bfloat16 [2304, 256], P('dp'), parts along dimension 0
- output 5: bfloat16 [2304, 256], P('dp'), parts along dimension 0
- output 6: bfloat16 [2048, 1152], P('dp'), parts along dimension 0
- output 7: float32 [2304], P('dp'), parts along dimension 0
- output 8: float32 [2304], P('dp'), parts along dimension 0
- output 9: float32 [512], P('dp'), parts along dimension 0
- output 10: float32 [512], P('dp'), parts along dimension 0
There are 2 independent parts. The reference program is written for one: setup_inputs(seed, part) draws one part's arguments, and reference() takes and returns one part's arrays. A program takes and returns all parts, laid end to end along the dimension named above; an argument that names none is the same for every part.
All inputs are finite; a program needn't handle non-finite values.
Results may differ from the reference program's by a relative error of at most 0.018656.
Values are sent between devices in bfloat16 or wider.
A program may use at most 1 GiB of HBM per device.

```python
import functools
import jax
import jax.numpy as jnp
from jax import lax

B = 8
SEQ = 4096
D = 1152
H = 4
K = 1
HEAD = 256

EPS = 1e-6
ROPE_BASE = 1000000.0
ROPE_SCALE = 8.0
NEG_BIG = -1e30
Q_ROWS = min(128, SEQ)


def setup_inputs(seed: int = 0, part: int = 0) -> dict:
    base_key = jax.random.key(seed)
    own = jax.random.split(jax.random.fold_in(base_key, part), 4)
    shared = jax.random.split(base_key, 8)
    x_in = jax.random.normal(own[0], (B, SEQ, D), jnp.float32).astype(jnp.bfloat16)
    dy_in = jax.random.normal(own[1], (B, SEQ, D), jnp.float32).astype(jnp.bfloat16)
    start = jax.random.randint(own[2], (1,), 0, 1000)
    gaps = jax.random.randint(own[3], (SEQ,), 1, 5)
    positions = (start + jnp.cumsum(gaps) - gaps[0]).astype(jnp.int32)
    w_q = (jax.random.normal(shared[0], (D, H * HEAD), jnp.float32) * D ** -0.5).astype(jnp.bfloat16)
    w_k = (jax.random.normal(shared[1], (D, K * HEAD), jnp.float32) * D ** -0.5).astype(jnp.bfloat16)
    w_v = (jax.random.normal(shared[2], (D, K * HEAD), jnp.float32) * D ** -0.5).astype(jnp.bfloat16)
    w_o = (jax.random.normal(shared[3], (H * HEAD, D), jnp.float32) * (H * HEAD) ** -0.5).astype(jnp.bfloat16)
    w_pre = 0.3 * jax.random.normal(shared[4], (D,), jnp.float32)
    w_post = 0.3 * jax.random.normal(shared[5], (D,), jnp.float32)
    q_norm = 0.3 + 0.3 * jax.random.normal(shared[6], (HEAD,), jnp.float32)
    k_norm = 0.3 + 0.3 * jax.random.normal(shared[7], (HEAD,), jnp.float32)
    return {'x_in': x_in, 'dy_in': dy_in, 'positions': positions, 'w_q': w_q, 'w_k': w_k, 'w_v': w_v, 'w_o': w_o, 'w_pre': w_pre, 'w_post': w_post, 'q_norm': q_norm, 'k_norm': k_norm}


def rms_scale(x_f32, weight):
    inv_rms = lax.rsqrt(jnp.mean(x_f32 * x_f32, axis=-1, keepdims=True) + EPS)
    return x_f32 * inv_rms * (1.0 + weight)


def norm_rope(heads_f32, weight, cosines, sines):
    half_dim = HEAD // 2
    normed = rms_scale(heads_f32, weight)
    first = normed[..., :half_dim]
    second = normed[..., half_dim:]
    cos_b = cosines[None, :, None, :]
    sin_b = sines[None, :, None, :]
    return jnp.concatenate([first * cos_b - second * sin_b, second * cos_b + first * sin_b], axis=-1)


def attention(q_rot, k_rot, v_heads):
    group = H // K
    blocks = SEQ // Q_ROWS
    q_blocks = jnp.moveaxis(q_rot.reshape(B, blocks, Q_ROWS, K, group, HEAD), 1, 0)
    key_f32 = k_rot.astype(jnp.float32)
    val_f32 = v_heads.astype(jnp.float32)
    col_ids = jnp.arange(SEQ)

    def one_block(item):
        q_blk, index = item
        scores = jnp.einsum('bqkgh,bskh->bkgqs', q_blk.astype(jnp.float32), key_f32) * HEAD ** -0.5
        row_ids = index * Q_ROWS + jnp.arange(Q_ROWS)
        scores = jnp.where(row_ids[:, None] >= col_ids[None, :], scores, NEG_BIG)
        attn_prob = jax.nn.softmax(scores, axis=-1).astype(jnp.bfloat16).astype(jnp.float32)
        return jnp.einsum('bkgqs,bskh->bqkgh', attn_prob, val_f32).astype(jnp.bfloat16)

    block_out = lax.map(jax.checkpoint(one_block), (q_blocks, jnp.arange(blocks)))
    return jnp.moveaxis(block_out, 0, 1).reshape(B, SEQ, H, HEAD)


def forward(positions, x_in, w_q, w_k, w_v, w_o, w_pre, w_post, q_norm, k_norm):
    x_f32 = x_in.astype(jnp.float32)
    normed = rms_scale(x_f32, w_pre).astype(jnp.bfloat16).astype(jnp.float32)
    q_proj = jnp.einsum('bsd,dn->bsn', normed, w_q.astype(jnp.float32)).astype(jnp.bfloat16)
    k_proj = jnp.einsum('bsd,dn->bsn', normed, w_k.astype(jnp.float32)).astype(jnp.bfloat16)
    v_proj = jnp.einsum('bsd,dn->bsn', normed, w_v.astype(jnp.float32)).astype(jnp.bfloat16)
    half_dim = HEAD // 2
    inv_freq = ROPE_BASE ** (-jnp.arange(half_dim, dtype=jnp.float32) * 2.0 / HEAD)
    angles = (positions.astype(jnp.float32) / ROPE_SCALE)[:, None] * inv_freq[None, :]
    cosines = jnp.cos(angles)
    sines = jnp.sin(angles)
    q_rot = norm_rope(q_proj.reshape(B, SEQ, H, HEAD).astype(jnp.float32), q_norm, cosines, sines).astype(jnp.bfloat16)
    k_rot = norm_rope(k_proj.reshape(B, SEQ, K, HEAD).astype(jnp.float32), k_norm, cosines, sines).astype(jnp.bfloat16)
    v_heads = v_proj.reshape(B, SEQ, K, HEAD)
    attn_out = attention(q_rot, k_rot, v_heads)
    proj = jnp.einsum('bsn,nd->bsd', attn_out.reshape(B, SEQ, H * HEAD).astype(jnp.float32), w_o.astype(jnp.float32)).astype(jnp.bfloat16)
    return (x_f32 + rms_scale(proj.astype(jnp.float32), w_post)).astype(jnp.bfloat16)


def reference(x_in, dy_in, positions, w_q, w_k, w_v, w_o, w_pre, w_post, q_norm, k_norm):
    y_out, pullback = jax.vjp(functools.partial(forward, positions), x_in, w_q, w_k, w_v, w_o, w_pre, w_post, q_norm, k_norm)
    grads = pullback(dy_in)
    return (y_out, grads[0], grads[1], grads[2], grads[3], grads[4], grads[5], grads[6], grads[7], grads[8])
```

```python
import functools
import jax
import jax.numpy as jnp
from jax import lax
from jax.experimental import pallas as pl
from jax.experimental.pallas import tpu as pltpu
from jax.sharding import PartitionSpec as P

EPS = 1e-6
ROPE_BASE = 1000000.0
ROPE_SCALE = 8.0
NEG_BIG = -1e30
BLOCK = 512
PAIR = 2
LOG2E = 1.4426950408889634
NT = (((1,), (1,)), ((), ()))
F32 = jnp.float32
BF16 = jnp.bfloat16


def rms_scale(x_f32, weight):
    inv_rms = lax.rsqrt(jnp.mean(x_f32 * x_f32, axis=-1, keepdims=True) + EPS)
    return x_f32 * inv_rms * (1.0 + weight)


def pre_norm(x_f32, weight):
    return rms_scale(x_f32, weight).astype(BF16)


def post_norm(proj, weight):
    return rms_scale(proj.astype(F32), weight)


def rope_tables(positions, head):
    half_dim = head // 2
    inv_freq = ROPE_BASE ** (-jnp.arange(half_dim, dtype=F32) * 2.0 / head)
    angles = (positions.astype(F32) / ROPE_SCALE)[:, None] * inv_freq[None, :]
    return jnp.cos(angles), jnp.sin(angles)


def rope_fwd_kernel(qkv_ref, cos_ref, sin_ref, qg_ref, kg_ref, q_ref, k_ref, kt_ref, vt_ref, *, heads, head):
    half = head // 2
    cos_b, sin_b = cos_ref[...], sin_ref[...]
    for h in range(heads + 1):
        cols = slice(h * head, (h + 1) * head)
        gain = qg_ref[...] if h < heads else kg_ref[...]
        normed = rms_scale(qkv_ref[:, cols].astype(F32), gain)
        first, second = normed[:, :half], normed[:, half:]
        rotated = jnp.concatenate([first * cos_b - second * sin_b, second * cos_b + first * sin_b], axis=-1)
        if h < heads:
            q_ref[:, cols] = rotated.astype(BF16)
        else:
            k_ref[...] = rotated.astype(BF16)
            kt_ref[...] = rotated.T.astype(BF16)
    vt_ref[...] = qkv_ref[:, (heads + 1) * head:].astype(F32).T.astype(BF16)


def rope_bwd_kernel(qkv_ref, dq_ref, dk_ref, dv_ref, cos_ref, sin_ref, qg_ref, kg_ref, dqkv_ref, dqg_ref, dkg_ref, *, heads, head):
    half = head // 2
    cos_b, sin_b = cos_ref[...], sin_ref[...]

    @pl.when(pl.program_id(0) == 0)
    def _():
        dqg_ref[...] = jnp.zeros_like(dqg_ref)
        dkg_ref[...] = jnp.zeros_like(dkg_ref)

    for h in range(heads + 1):
        cols = slice(h * head, (h + 1) * head)
        gain = 1.0 + (qg_ref[...] if h < heads else kg_ref[...])
        d_rot = (dq_ref[:, cols] if h < heads else dk_ref[...]).astype(F32)
        first, second = d_rot[:, :half], d_rot[:, half:]
        d_normed = jnp.concatenate([first * cos_b + second * sin_b, second * cos_b - first * sin_b], axis=-1)
        x_f32 = qkv_ref[:, cols].astype(F32)
        inv_rms = lax.rsqrt(jnp.mean(x_f32 * x_f32, axis=-1, keepdims=True) + EPS)
        unit = x_f32 * inv_rms
        d_gain = jnp.sum(d_normed * unit, axis=0, keepdims=True)
        if h < heads:
            dqg_ref[...] += d_gain
        else:
            dkg_ref[...] += d_gain
        d_unit = d_normed * gain
        d_x = inv_rms * (d_unit - unit * jnp.mean(d_unit * unit, axis=-1, keepdims=True))
        dqkv_ref[:, cols] = d_x.astype(BF16)
    dqkv_ref[:, (heads + 1) * head:] = dv_ref[...]


def rope_specs(block, heads, head):
    tall = lambda cols: pl.BlockSpec((block, cols), lambda i: (i, 0))
    flat = pl.BlockSpec((head, block), lambda i: (0, i))
    fixed = pl.BlockSpec((1, head), lambda i: (0, 0))
    return tall, flat, fixed


def rope_fwd(qkv, cosines, sines, q_gain, k_gain, heads, head):
    seq, wide = qkv.shape
    block = min(BLOCK, seq)
    tall, flat, fixed = rope_specs(block, heads, head)
    return pl.pallas_call(
        functools.partial(rope_fwd_kernel, heads=heads, head=head),
        grid=(seq // block,),
        in_specs=[tall(wide), tall(head // 2), tall(head // 2), fixed, fixed],
        out_specs=[tall(heads * head), tall(head), flat, flat],
        out_shape=[
            jax.ShapeDtypeStruct((seq, heads * head), BF16),
            jax.ShapeDtypeStruct((seq, head), BF16),
            jax.ShapeDtypeStruct((head, seq), BF16),
            jax.ShapeDtypeStruct((head, seq), BF16),
        ],
        compiler_params=pltpu.CompilerParams(dimension_semantics=('arbitrary',), vmem_limit_bytes=40 * 2 ** 20),
        cost_estimate=pl.CostEstimate(flops=20 * seq * wide, bytes_accessed=4 * seq * wide, transcendentals=seq),
        name='rope_fwd',
    )(qkv, cosines, sines, q_gain, k_gain)


def rope_bwd(qkv, dq, dk, dv, cosines, sines, q_gain, k_gain, heads, head):
    seq, wide = qkv.shape
    block = min(BLOCK, seq)
    tall, flat, fixed = rope_specs(block, heads, head)
    return pl.pallas_call(
        functools.partial(rope_bwd_kernel, heads=heads, head=head),
        grid=(seq // block,),
        in_specs=[tall(wide), tall(heads * head), tall(head), tall(head), tall(head // 2), tall(head // 2), fixed, fixed],
        out_specs=[tall(wide), fixed, fixed],
        out_shape=[
            jax.ShapeDtypeStruct((seq, wide), BF16),
            jax.ShapeDtypeStruct((1, head), F32),
            jax.ShapeDtypeStruct((1, head), F32),
        ],
        compiler_params=pltpu.CompilerParams(dimension_semantics=('arbitrary',), vmem_limit_bytes=40 * 2 ** 20),
        cost_estimate=pl.CostEstimate(flops=30 * seq * wide, bytes_accessed=6 * seq * wide, transcendentals=seq),
        name='rope_bwd',
    )(qkv, dq, dk, dv, cosines, sines, q_gain, k_gain)


def below_diagonal(block):
    keys = lax.broadcasted_iota(jnp.int32, (block, block), 0)
    queries = lax.broadcasted_iota(jnp.int32, (block, block), 1)
    return keys <= queries


def fwd_kernel(q_ref, k_ref, vt_ref, o_ref, lse_ref, acc, top, total, *, block, head):
    index = pl.program_id(0)
    mult = LOG2E * head ** -0.5

    def step(j, first):
        start = pl.multiple_of(j * block, block)
        keys = k_ref[pl.ds(start, block), :]
        vals = vt_ref[:, pl.ds(start, block)]
        for h in range(PAIR):
            query = q_ref[:, h * head:(h + 1) * head]
            scores = lax.dot_general(keys, query, NT, preferred_element_type=F32) * mult
            if first:
                scores = jnp.where(below_diagonal(block), scores, NEG_BIG)
                peak = jnp.max(scores, axis=0, keepdims=True)
                prob = jnp.exp2(scores - peak)
                total[h] = jnp.sum(prob, axis=0, keepdims=True)
                acc[h] = jnp.dot(vals, prob.astype(BF16), preferred_element_type=F32)
            else:
                old = top[h]
                peak = jnp.maximum(old, jnp.max(scores, axis=0, keepdims=True))
                prob = jnp.exp2(scores - peak)
                fade = jnp.exp2(old - peak)
                total[h] = total[h] * fade + jnp.sum(prob, axis=0, keepdims=True)
                acc[h] = acc[h] * fade + jnp.dot(vals, prob.astype(BF16), preferred_element_type=F32)
            top[h] = peak

    step(index, True)

    @pl.loop(0, index)
    def _(j):
        step(j, False)

    for h in range(PAIR):
        out = acc[h] / total[h]
        o_ref[:, h * head:(h + 1) * head] = out.T.astype(BF16)
        lse_ref[h] = top[h] + jnp.log2(total[h])


def bwd_kernel(q_ref, do_ref, lse_ref, delta_ref, k_ref, v_ref, kt_ref, dq_ref, dk_ref, dv_ref, dk_acc, dv_acc, dqt, *, block, head):
    index = pl.program_id(0)
    pair = pl.program_id(1)
    scale = head ** -0.5
    mult = LOG2E * scale

    @pl.when((index == 0) & (pair == 0))
    def _():
        dk_acc[...] = jnp.zeros_like(dk_acc)
        dv_acc[...] = jnp.zeros_like(dv_acc)

    def step(j, first):
        start = pl.multiple_of(j * block, block)
        rows = pl.ds(start, block)
        keys = k_ref[rows, :]
        vals = v_ref[rows, :]
        keys_t = kt_ref[:, rows]
        dk_part = []
        dv_part = []
        for h in range(PAIR):
            cols = slice(h * head, (h + 1) * head)
            query = q_ref[:, cols]
            d_out = do_ref[:, cols]
            scores = lax.dot_general(keys, query, NT, preferred_element_type=F32)
            prob = jnp.exp2(scores * mult - lse_ref[h])
            if first:
                prob = jnp.where(below_diagonal(block), prob, 0.0)
            d_prob = lax.dot_general(vals, d_out, NT, preferred_element_type=F32)
            d_score = (prob * (d_prob - delta_ref[h])).astype(BF16)
            dv_part.append(jnp.dot(prob.astype(BF16), d_out, preferred_element_type=F32))
            dk_part.append(jnp.dot(d_score, query, preferred_element_type=F32))
            dq_part = jnp.dot(keys_t, d_score, preferred_element_type=F32)
            if first:
                dqt[h] = dq_part
            else:
                dqt[h] += dq_part
        dk_acc[rows, :] += sum(dk_part)
        dv_acc[rows, :] += sum(dv_part)

    step(index, True)

    @pl.loop(0, index)
    def _(j):
        step(j, False)

    for h in range(PAIR):
        dq_ref[:, h * head:(h + 1) * head] = (dqt[h].T * scale).astype(BF16)

    @pl.when((index == pl.num_programs(0) - 1) & (pair == pl.num_programs(1) - 1))
    def _():
        dk_ref[...] = (dk_acc[...] * scale).astype(BF16)
        dv_ref[...] = dv_acc[...].astype(BF16)


def attention_fwd(q, k, v_t, head):
    seq, wide = q.shape
    heads = wide // head
    block = min(BLOCK, seq)
    flops = 2 * 2 * heads * seq * (seq + block) // 2 * head
    whole = lambda *_: (0, 0)
    return pl.pallas_call(
        functools.partial(fwd_kernel, block=block, head=head),
        grid=(seq // block, heads // PAIR),
        in_specs=[
            pl.BlockSpec((block, PAIR * head), lambda i, p: (i, p)),
            pl.BlockSpec((seq, head), whole),
            pl.BlockSpec((head, seq), whole),
        ],
        out_specs=[
            pl.BlockSpec((block, PAIR * head), lambda i, p: (i, p)),
            pl.BlockSpec((PAIR, 1, block), lambda i, p: (p, 0, i)),
        ],
        out_shape=[
            jax.ShapeDtypeStruct((seq, wide), BF16),
            jax.ShapeDtypeStruct((heads, 1, seq), F32),
        ],
        scratch_shapes=[
            pltpu.VMEM((PAIR, head, block), F32),
            pltpu.VMEM((PAIR, 1, block), F32),
            pltpu.VMEM((PAIR, 1, block), F32),
        ],
        compiler_params=pltpu.CompilerParams(
            dimension_semantics=('arbitrary', 'arbitrary'), vmem_limit_bytes=48 * 2 ** 20),
        cost_estimate=pl.CostEstimate(flops=flops, bytes_accessed=4 * seq * wide, transcendentals=heads * seq * seq // 2),
        name='attn_fwd',
    )(q, k, v_t)


def attention_bwd(q, k, k_t, qkv, lse, d_out, delta, head):
    seq, wide = q.shape
    heads = wide // head
    block = min(BLOCK, seq)
    flops = 5 * 2 * heads * seq * (seq + block) // 2 * head
    whole = lambda *_: (0, 0)
    wide_spec = pl.BlockSpec((block, PAIR * head), lambda i, p: (i, p))
    row_spec = pl.BlockSpec((PAIR, 1, block), lambda i, p: (p, 0, i))
    return pl.pallas_call(
        functools.partial(bwd_kernel, block=block, head=head),
        grid=(seq // block, heads // PAIR),
        in_specs=[
            wide_spec, wide_spec, row_spec, row_spec,
            pl.BlockSpec((seq, head), whole),
            pl.BlockSpec((seq, head), lambda *_: (0, heads + 1)),
            pl.BlockSpec((head, seq), whole),
        ],
        out_specs=[wide_spec, pl.BlockSpec((seq, head), whole), pl.BlockSpec((seq, head), whole)],
        out_shape=[
            jax.ShapeDtypeStruct((seq, wide), BF16),
            jax.ShapeDtypeStruct((seq, head), BF16),
            jax.ShapeDtypeStruct((seq, head), BF16),
        ],
        scratch_shapes=[
            pltpu.VMEM((seq, head), F32),
            pltpu.VMEM((seq, head), F32),
            pltpu.VMEM((PAIR, head, block), F32),
        ],
        compiler_params=pltpu.CompilerParams(
            dimension_semantics=('arbitrary', 'arbitrary'), vmem_limit_bytes=56 * 2 ** 20),
        cost_estimate=pl.CostEstimate(flops=flops, bytes_accessed=6 * seq * wide, transcendentals=heads * seq * seq // 2),
        name='attn_bwd',
    )(q, d_out, lse, delta, k, qkv, k_t)


def matmul(a, b):
    return jnp.dot(a, b, preferred_element_type=F32)


def solution(mesh):
    group = mesh.shape['sp']

    def exchange(arr):
        return lax.all_to_all(arr, 'sp', 0, 0, tiled=True)

    def spread_sum(grad):
        part = lax.psum_scatter(grad, 'sp', scatter_dimension=0, tiled=True)
        return lax.all_gather(part.astype(BF16), 'sp', axis=0, tiled=True)

    def device_step(x_in, dy_in, positions, w_q, w_k, w_v, w_o, w_pre, w_post, q_norm, k_norm):
        batch, seq_loc, width = x_in.shape
        head = q_norm.shape[0]
        heads = w_q.shape[1] // head
        q_wide = heads * head
        seq = group * seq_loc
        rounds = batch // group
        x_seqs = [exchange(x_in[r * group:(r + 1) * group]).reshape(seq, width) for r in range(rounds)]
        dy_seqs = [exchange(dy_in[r * group:(r + 1) * group]).reshape(seq, width) for r in range(rounds)]
        pos_all = lax.all_gather(positions, 'sp', axis=0, tiled=True)
        cosines, sines = rope_tables(pos_all, head)
        gains = (q_norm[None, :], k_norm[None, :])
        w_qkv = jnp.concatenate([w_q, w_k, w_v], axis=1)
        cut = lambda arr, h: arr[:, h * head:(h + 1) * head]

        y_parts, saved = [], []
        dw_o = dw_post = 0.0
        for r in range(rounds):
            x_f32 = x_seqs[r].astype(F32)
            normed, pre_pull = jax.vjp(pre_norm, x_f32, w_pre)
            qkv = matmul(normed, w_qkv).astype(BF16)
            q_rot, k_rot, k_t, v_t = rope_fwd(qkv, cosines, sines, *gains, heads, head)
            o_flat, lse = attention_fwd(q_rot, k_rot, v_t, head)
            proj = matmul(o_flat, w_o).astype(BF16)
            post, post_pull = jax.vjp(post_norm, proj, w_post)
            y_parts.append(exchange((x_f32 + post).astype(BF16).reshape(group, seq_loc, width)))
            dy_f32 = dy_seqs[r].astype(F32)
            d_proj, dw_post_r = post_pull(dy_f32)
            dw_post += dw_post_r
            dw_o += lax.dot_general(o_flat, d_proj, (((0,), (0,)), ((), ())), preferred_element_type=F32)
            d_oflat = lax.dot_general(d_proj, w_o, NT, preferred_element_type=F32).astype(BF16)
            delta = jnp.stack([jnp.sum(cut(d_oflat, h).astype(F32) * cut(o_flat, h).astype(F32), axis=-1) for h in range(heads)])[:, None, :]
            saved.append((normed, pre_pull, qkv, q_rot, k_rot, k_t, lse, d_oflat, delta, dy_f32))
        dw_o = spread_sum(dw_o)

        dx_parts = []
        dw_qkv = dw_pre = dq_norm = dk_norm = 0.0
        for r in range(rounds):
            normed, pre_pull, qkv, q_rot, k_rot, k_t, lse, d_oflat, delta, dy_f32 = saved[r]
            dq_rot, dk_rot, dv_proj = attention_bwd(q_rot, k_rot, k_t, qkv, lse, d_oflat, delta, head)
            d_qkv, d_qg, d_kg = rope_bwd(qkv, dq_rot, dk_rot, dv_proj, cosines, sines, *gains, heads, head)
            dq_norm += d_qg[0]
            dk_norm += d_kg[0]
            d_normed = lax.dot_general(d_qkv, w_qkv, NT, preferred_element_type=F32).astype(BF16)
            dx_norm, dw_pre_r = pre_pull(d_normed)
            dw_pre += dw_pre_r
            dx_parts.append(exchange((dy_f32 + dx_norm).astype(BF16).reshape(group, seq_loc, width)))
            dw_qkv += lax.dot_general(normed, d_qkv, (((0,), (0,)), ((), ())), preferred_element_type=F32)
        dw_qkv = spread_sum(dw_qkv)
        kv_wide = w_k.shape[1]
        sums = lax.psum((dw_pre, dw_post, dq_norm, dk_norm), 'sp')
        return (jnp.concatenate(y_parts, axis=0), jnp.concatenate(dx_parts, axis=0),
                dw_qkv[:, :q_wide], dw_qkv[:, q_wide:q_wide + kv_wide], dw_qkv[:, q_wide + kv_wide:], dw_o) + sums

    token_spec = P('dp', 'sp', None)
    return jax.shard_map(device_step, mesh=mesh,
                         in_specs=(token_spec, token_spec, P(('dp', 'sp')), P(None, None), P(None, None), P(None, None), P(None, None), P(None), P(None), P(None), P(None)),
                         out_specs=(token_spec, token_spec, P('dp', None), P('dp', None), P('dp', None), P('dp', None), P('dp'), P('dp'), P('dp'), P('dp')),
                         check_vma=False)
```
